32 devices in a mesh: grp: 4 (over y, core), dp: 8 (over z, x).
Axes of the slice: x: 2, y: 2, z: 4, core: 2. Of those that a mesh axis runs over, the one named last changes fastest.
Arguments:
- tokens: bfloat16 [4, 1024, 2048], P('grp', 'dp'), may hold values from -6 to 6
- hidden_grad: bfloat16 [4, 1024, 6144], P('grp', 'dp'), may hold values from -6 to 6
- w_gate: bfloat16 [4, 2048, 6144], P('grp', None, 'dp'), may hold values from -6 to 6
- w_up: bfloat16 [4, 2048, 6144], P('grp', None, 'dp'), may hold values from -6 to 6
Outputs:
- mixed_gate: bfloat16 [4, 2048, 6144], P('grp', None, 'dp')
- mixed_up: bfloat16 [4, 2048, 6144], P('grp', None, 'dp')
The draws below stay inside these ranges and needn't reach their ends.
All inputs are finite; a program needn't handle non-finite values.
Results may differ from the reference program's by a relative error of at most 0.0052.
Values may be sent and summed in bfloat16 or wider, within the bound.
A program may use at most 256 MiB of HBM per device.

```python
import jax
import jax.numpy as jnp
from jax import lax

D = 2048
FF = 6144
GROUPS = 4
GROUP_TOKENS = 1024


def level_of(rng, shape, cuts, smallest, high):
    def one(axis_at, parts):
        heights = jax.random.uniform(jax.random.fold_in(jax.random.fold_in(rng, 6), axis_at), (parts,), jnp.float32, smallest / len(cuts), high / len(cuts))
        return jnp.repeat(jnp.exp(heights), shape[axis_at] // parts).reshape((-1,) + (1,) * (len(shape) - axis_at - 1))

    loudness = one(*cuts[0])
    for cut in cuts[1:]:
        loudness = loudness * one(*cut)
    return loudness


def scatter_about(key, dims, spread, reach, cuts=(), kind=jnp.bfloat16):
    drawn = jax.random.normal(key, dims, jnp.float32) * spread
    if len(cuts) > 0:
        drawn = level_of(key, dims, cuts, -0.22, 0.18) * drawn
    return jnp.clip(drawn, min=-reach, max=reach).astype(kind)


def setup_inputs(seed: int = 0) -> dict:
    key_of = jax.random.split(jax.random.key(seed), 5)
    tokens = scatter_about(key_of[0], (GROUPS, GROUP_TOKENS, D), 1.0, 6.0, ((0, 4), (1, 8)))
    hidden_grad = scatter_about(key_of[1], (GROUPS, GROUP_TOKENS, FF), 1.0, 6.0, ((0, 4), (1, 8)))
    w_gate = scatter_about(key_of[2], (GROUPS, D, FF), 1.0, 6.0, ((0, 4), (2, 8)))
    w_up = scatter_about(key_of[3], (GROUPS, D, FF), 1.0, 6.0, ((0, 4), (2, 8)))
    return dict(tokens=tokens, hidden_grad=hidden_grad, w_gate=w_gate, w_up=w_up)


def one_replica(operands):
    rows, cotangent, gate_weight, up_weight = operands
    scale = D ** -0.5
    gate = jnp.dot(rows, gate_weight, preferred_element_type=jnp.float32) * scale
    up = jnp.dot(rows, up_weight, preferred_element_type=jnp.float32) * scale
    sigma = jax.nn.sigmoid(gate)
    upstream = cotangent.astype(jnp.float32)
    gate_rows = (upstream * up * sigma * (1.0 + gate * (1.0 - sigma))).astype(jnp.bfloat16)
    up_rows = (upstream * gate * sigma).astype(jnp.bfloat16)
    gate_grad = jnp.dot(rows.T, gate_rows, preferred_element_type=jnp.float32) * scale
    up_grad = jnp.dot(rows.T, up_rows, preferred_element_type=jnp.float32) * scale
    gate_step = (gate_weight.astype(jnp.float32) - 0.5 * gate_grad).astype(jnp.bfloat16)
    up_step = (up_weight.astype(jnp.float32) - 0.5 * up_grad).astype(jnp.bfloat16)
    return gate_step, up_step


def average_cycle(stepped):
    wide = stepped.astype(jnp.float32)
    mixed = 0.5 * wide + 0.25 * (jnp.roll(wide, 1, axis=0) + jnp.roll(wide, -1, axis=0))
    return mixed.astype(jnp.bfloat16)


def reference(tokens, hidden_grad, w_gate, w_up):
    gate_step, up_step = lax.map(one_replica, (tokens, hidden_grad, w_gate, w_up))
    return average_cycle(gate_step), average_cycle(up_step)
```

```python
import jax
import jax.numpy as jnp
from jax import lax
from jax.sharding import PartitionSpec as P

LANES = 128


def near_pairs(size):
    return [(i, i ^ 1) for i in range(size)]


def far_pairs(size):
    return [(i, (i + 1) % size if i % 2 else (i - 1) % size) for i in range(size)]


def stepped(rows, cotangent, gate_weight, up_weight):
    scale = rows.shape[1] ** (-0.5)
    gate = jnp.dot(rows, gate_weight, preferred_element_type=jnp.float32) * scale
    up = jnp.dot(rows, up_weight, preferred_element_type=jnp.float32) * scale
    sigma = jax.nn.sigmoid(gate)
    upstream = cotangent.astype(jnp.float32)
    gate_rows = (upstream * up * sigma * (1.0 + gate * (1.0 - sigma))).astype(jnp.bfloat16)
    up_rows = (upstream * gate * sigma).astype(jnp.bfloat16)

    def step(weight, unit_rows):
        gradient = jnp.dot(rows.T, unit_rows, preferred_element_type=jnp.float32) * scale
        return (weight.astype(jnp.float32) - 0.5 * gradient).astype(jnp.bfloat16)

    return step(gate_weight, gate_rows), step(up_weight, up_rows)


def average(own, near, far):
    mixed = 0.5 * own.astype(jnp.float32) + 0.25 * (near.astype(jnp.float32) + far.astype(jnp.float32))
    return mixed.astype(jnp.bfloat16)


def local(tokens, hidden_grad, w_gate, w_up):
    groups = lax.axis_size("grp")
    far = lambda x: lax.ppermute(x, "grp", far_pairs(groups))
    near = lambda x: lax.ppermute(x, "grp", near_pairs(groups))
    rows, gate_weight, up_weight = tokens[0], w_gate[0], w_up[0]
    units = gate_weight.shape[1]
    cut = 2 * (units // LANES) // 3 * LANES
    far_shard = far(rows)
    far_gate_weight = far(gate_weight[:, :cut])
    far_up_weight = far(up_weight[:, :cut])
    cotangent = lax.all_to_all(hidden_grad[0], "dp", split_axis=1, concat_axis=0, tiled=True)
    gathered = lax.all_gather(rows, "dp", axis=0, tiled=True)
    far_cotangent = far(cotangent[:, :cut])
    last = stepped(gathered, cotangent[:, cut:], gate_weight[:, cut:], up_weight[:, cut:])
    far_last = [far(x) for x in last]
    first = stepped(gathered, cotangent[:, :cut], gate_weight[:, :cut], up_weight[:, :cut])
    near_last = [near(x) for x in last]
    near_first = [near(x) for x in first]
    far_gathered = lax.all_gather(far_shard, "dp", axis=0, tiled=True)
    far_first = stepped(far_gathered, far_cotangent, far_gate_weight, far_up_weight)
    outs = []
    for k in range(2):
        left = average(first[k], near_first[k], far_first[k])
        right = average(last[k], near_last[k], far_last[k])
        outs.append(jnp.concatenate([left, right], axis=1)[None])
    return tuple(outs)


def solution(mesh):
    in_specs = (
        P("grp", "dp", None),
        P("grp", "dp", None),
        P("grp", None, "dp"),
        P("grp", None, "dp"),
    )
    out_specs = (P("grp", None, "dp"), P("grp", None, "dp"))
    return jax.shard_map(local, mesh=mesh, in_specs=in_specs, out_specs=out_specs, check_vma=False)
```
